32 devices in a mesh: space: 8 (over y, x, core), tm: 4 (over z).
Axes of the slice: x: 2, y: 2, z: 4, core: 2. Of those that a mesh axis runs over, the one named last changes fastest.
Arguments:
- links: float32 [4, 3, 2, 3, 3, 16, 4096], P('tm', None, None, None, None, 'space'), may hold values from -1 to 1, as said below
- propagator: float32 [2, 144, 16, 4096], P(None, 'tm', 'space'), may hold values from -6 to 6
- sink_time: int32 [1], replicated, may hold values from 0 to 16383
- src_time: int32 [1], replicated, may hold values from 0 to 16383
- src_site: int32 [1], replicated, may hold values from 0 to 65535
Outputs:
- fixed_links: float32 [4, 3, 2, 3, 3, 16, 4096], P('tm', None, None, None, None, 'space')
- wall: float32 [2, 144], replicated
The draws below stay inside these ranges and needn't reach their ends.
Inputs may be any that keep to these rules, and one draw needn't show every extreme that they name: `links`: every link is a special unitary 3 x 3 matrix up to rounding.
All inputs are finite; a program needn't handle non-finite values.
Results may differ from the reference program's by a relative error of at most 0.0001.
Values sent between devices are 32-bit elements; how exact they have to be, the bound alone decides.
A program may use at most 128 MiB of HBM per device.

```python
import math
import jax
import jax.numpy as jnp
from jax import lax

L = 64
SC = 12
ITERS = 2
NX = 16
NT = 4


def draw_product(left_matrix, right_matrix):
    pattern = 'tdikxn,tdkjxn->tdijxn'
    real_part = jnp.einsum(pattern, left_matrix[:, :, 0], right_matrix[:, :, 0]) - jnp.einsum(pattern, left_matrix[:, :, 1], right_matrix[:, :, 1])
    imag_part = jnp.einsum(pattern, left_matrix[:, :, 0], right_matrix[:, :, 1]) + jnp.einsum(pattern, left_matrix[:, :, 1], right_matrix[:, :, 0])
    return jnp.stack([real_part, imag_part], axis=2)


def draw_links(key, part):
    normal_draw = jax.random.normal(key, (NT, 3, 2, 3, 3, NX, L * L), jnp.float32)
    real_part = normal_draw[:, :, 0]
    imag_part = normal_draw[:, :, 1]
    real_anti = 0.5 * (real_part - jnp.swapaxes(real_part, 2, 3))
    imag_sym = 0.5 * (imag_part + jnp.swapaxes(imag_part, 2, 3))
    trace_third = (imag_sym[:, :, 0, 0] + imag_sym[:, :, 1, 1] + imag_sym[:, :, 2, 2]) / 3.0
    unit_matrix = jnp.eye(3, dtype=jnp.float32)[None, None, :, :, None, None]
    imag_sym = imag_sym - unit_matrix * trace_third[:, :, None, None]
    algebra = jnp.stack([real_anti, imag_sym], axis=2) / 16.0
    identity = jnp.stack([jnp.broadcast_to(unit_matrix, real_anti.shape), jnp.zeros(real_anti.shape, jnp.float32)], axis=2)
    result = identity
    for degree in range(8, 0, -1):
        result = identity + draw_product(algebra, result) / degree
    for square_index in range(4):
        result = draw_product(result, result)
    return result


def level_of(rng, extent, shards, least, largest):
    def one(axis_at, shards_of):
        heights = jax.random.uniform(jax.random.fold_in(jax.random.fold_in(rng, 6), axis_at), (shards_of,), jnp.float32, least / len(shards), largest / len(shards))
        return jnp.repeat(jnp.exp(heights), extent[axis_at] // shards_of).reshape((-1,) + (1,) * (len(extent) - axis_at - 1))

    level = one(*shards[0])
    for cut in shards[1:]:
        level = level * one(*cut)
    return level


def noise(key, shape, scale, reach, cuts=(), kind=jnp.bfloat16):
    entries = scale * jax.random.normal(key, shape, jnp.float32)
    if cuts:
        entries = entries * level_of(key, shape, cuts, -0.22, 0.18)
    return jnp.clip(entries, -reach, reach).astype(kind)


def setup_inputs(seed: int = 0) -> dict:
    arg_keys = jax.random.split(jax.random.key(seed), 6)
    links = draw_links(jax.random.fold_in(arg_keys[5], 71), 0)
    propagator = noise(arg_keys[1], (2, SC * SC, NX, L * L), 1.0, 6.0, ((1, 4), (2, 8)), jnp.float32)
    sink_time = jax.random.randint(arg_keys[2], (1,), 0, NT * 4096).astype(jnp.int32)
    src_time = jax.random.randint(arg_keys[3], (1,), 0, NT * 4096).astype(jnp.int32)
    src_site = jax.random.randint(arg_keys[4], (1,), 0, NX * L * L).astype(jnp.int32)
    return dict(links=links, propagator=propagator, sink_time=sink_time, src_time=src_time, src_site=src_site)


STEP_SIZE = 0.08
PEAK_SQUARE = 12.0
ENTRY_PAIRS = ((0, 0), (0, 1), (0, 2), (1, 1), (1, 2), (2, 2))
EXACT = lax.Precision.HIGHEST


def colour_product(left_matrix, right_matrix):
    return jnp.sum(left_matrix[:, :, None] * right_matrix[None, :, :], axis=1)


def complex_product(left_matrix, right_matrix):
    real_part = colour_product(left_matrix[0], right_matrix[0]) - colour_product(left_matrix[1], right_matrix[1])
    imag_part = colour_product(left_matrix[0], right_matrix[1]) + colour_product(left_matrix[1], right_matrix[0])
    return jnp.stack([real_part, imag_part])


def dagger(matrix):
    return jnp.stack([jnp.swapaxes(matrix[0], 0, 1), -jnp.swapaxes(matrix[1], 0, 1)])


def roll_depth(values, amount):
    old_shape = values.shape
    folded = values.reshape(old_shape[:-1] + (L, L))
    return jnp.roll(folded, amount, axis=-1).reshape(old_shape)


def project(divergence):
    real_part = 0.5 * (divergence[0] - jnp.swapaxes(divergence[0], 0, 1))
    imag_part = 0.5 * (divergence[1] + jnp.swapaxes(divergence[1], 0, 1))
    trace_third = (imag_part[0, 0] + imag_part[1, 1] + imag_part[2, 2]) / 3.0
    real_six = jnp.stack([real_part[row_index, column_index] for row_index, column_index in ENTRY_PAIRS])
    imag_six = jnp.stack([imag_part[row_index, column_index] - trace_third if row_index == column_index else imag_part[row_index, column_index] for row_index, column_index in ENTRY_PAIRS])
    return real_six, imag_six


def assemble(real_six, imag_six):
    zero_plane = jnp.zeros_like(real_six[0])
    position = {}
    for entry_index, entry_pair in enumerate(ENTRY_PAIRS):
        position[entry_pair] = entry_index
    real_rows = []
    imag_rows = []
    for row_index in range(3):
        real_line = []
        imag_line = []
        for column_index in range(3):
            if row_index == column_index:
                real_line.append(zero_plane)
                imag_line.append(imag_six[position[(row_index, row_index)]])
            elif row_index < column_index:
                slot_index = position[(row_index, column_index)]
                real_line.append(real_six[slot_index])
                imag_line.append(imag_six[slot_index])
            else:
                slot_index = position[(column_index, row_index)]
                real_line.append(-real_six[slot_index])
                imag_line.append(imag_six[slot_index])
        real_rows.append(jnp.stack(real_line))
        imag_rows.append(jnp.stack(imag_line))
    return jnp.stack([jnp.stack(real_rows), jnp.stack(imag_rows)])


def exponential(algebra):
    unit_matrix = jnp.eye(3, dtype=jnp.float32).reshape((3, 3) + (1,) * (algebra.ndim - 3))
    identity = jnp.stack([jnp.broadcast_to(unit_matrix, algebra.shape[1:]), jnp.zeros(algebra.shape[1:], jnp.float32)])
    result = identity
    for degree in range(6, 0, -1):
        result = identity + complex_product(algebra, result) / degree
    for square_index in range(3):
        result = complex_product(result, result)
    return result


def rotate(lattice, gauge_field, gauge_ahead):
    along_x = complex_product(complex_product(gauge_field, lattice[0]), dagger(gauge_ahead))
    along_y = complex_product(complex_product(gauge_field, lattice[1]), dagger(jnp.roll(gauge_field, -L, axis=4)))
    along_z = complex_product(complex_product(gauge_field, lattice[2]), dagger(roll_depth(gauge_field, -1)))
    return jnp.stack([along_x, along_y, along_z])


def sink_product(gauge_field, propagator):
    pair_count = propagator.shape[1]
    source = propagator.reshape((2, pair_count // 3, 3) + propagator.shape[2:])
    pattern = "acxn,qcxn->qa"
    real_part = jnp.einsum(pattern, gauge_field[0], source[0], precision=EXACT) - jnp.einsum(pattern, gauge_field[1], source[1], precision=EXACT)
    imag_part = jnp.einsum(pattern, gauge_field[0], source[1], precision=EXACT) + jnp.einsum(pattern, gauge_field[1], source[0], precision=EXACT)
    return jnp.stack([real_part.reshape(pair_count), imag_part.reshape(pair_count)])


def source_rotate(wall_total, anchor):
    by_spin = wall_total.reshape(2, 4, 3, SC)
    pattern = "scn,bc->sbn"
    real_part = jnp.einsum(pattern, by_spin[0], anchor[0], precision=EXACT) + jnp.einsum(pattern, by_spin[1], anchor[1], precision=EXACT)
    imag_part = jnp.einsum(pattern, by_spin[1], anchor[0], precision=EXACT) - jnp.einsum(pattern, by_spin[0], anchor[1], precision=EXACT)
    return jnp.stack([real_part.reshape(SC * SC), imag_part.reshape(SC * SC)])


def sine_squares(length):
    wavenumber = jnp.arange(length, dtype=jnp.float32)
    return 4.0 * jnp.sin(math.pi * wavenumber / length) ** 2


def inverse_square():
    across = sine_squares(NX)
    sine_square = sine_squares(L)
    momentum = across[:, None, None] + sine_square[None, :, None] + sine_square[None, None, :]
    guarded = jnp.where(momentum > 0.0, momentum, 1.0)
    return jnp.where(momentum > 0.0, PEAK_SQUARE / guarded, 0.0)


def reference(links, propagator, sink_time, src_time, src_site):
    filter_weight = inverse_square()

    def fix_timeslice(lattice):
        overall = None
        for sweep_index in range(ITERS):
            divergence = jnp.roll(lattice[0], 1, axis=3) - lattice[0] + jnp.roll(lattice[1], L, axis=4) - lattice[1] + roll_depth(lattice[2], 1) - lattice[2]
            real_six, imag_six = project(divergence)
            packed = (real_six + 1j * imag_six).reshape(6, NX, L, L)
            spectrum = jnp.fft.fftn(packed, axes=(1, 2, 3)) * filter_weight[None]
            filtered = jnp.fft.ifftn(spectrum, axes=(1, 2, 3)).reshape(6, NX, L * L)
            algebra = assemble(jnp.real(filtered), jnp.imag(filtered))
            gauge_field = exponential(algebra * (STEP_SIZE / 16.0))
            lattice = rotate(lattice, gauge_field, jnp.roll(gauge_field, -1, axis=3))
            overall = gauge_field if overall is None else complex_product(gauge_field, overall)
        return lattice, overall

    fixed_links, overall_all = lax.map(fix_timeslice, links)
    sink_slice = sink_time[0] % NT
    source_slice = src_time[0] % NT
    wall_total = sink_product(overall_all[sink_slice], propagator)
    site_index = src_site[0]
    anchor = overall_all[source_slice][:, :, :, site_index // (L * L), site_index % (L * L)]
    wall = source_rotate(wall_total, anchor) * float(NX * L * L) ** -0.5
    return fixed_links, wall
```

```python
import functools
import math

import jax
import jax.numpy as jnp
import numpy as np
from jax import lax
from jax.experimental import pallas as pl
from jax.experimental.pallas import tpu as pltpu
from jax.sharding import PartitionSpec as P

SC = 12
ITERS = 2
STEP = 0.08 / 16.0
PEAK = 12.0
LANES = 128
FIELDS = 8
EXACT = lax.Precision.HIGHEST
MESH = pl.DeviceIdType.MESH
VMEM = pl.BlockSpec(memory_space=pltpu.VMEM)
SMEM = pl.BlockSpec(memory_space=pltpu.SMEM)
LIMIT = 60 * 1024 * 1024


def real_basis(n):
    x = np.arange(n)
    rows, moment = [], []
    for k in range(n // 2 + 1):
        angle = 2.0 * np.pi * ((k * x) % n) / n
        square = 4.0 * np.sin(np.pi * k / n) ** 2
        if k == 0 or 2 * k == n:
            rows.append(np.cos(angle) / np.sqrt(n))
            moment.append(square)
        else:
            rows.append(np.cos(angle) * np.sqrt(2.0 / n))
            rows.append(np.sin(angle) * np.sqrt(2.0 / n))
            moment += [square, square]
    return np.array(rows), np.array(moment)


def plane_matrices(q):
    n = q.shape[0]
    zero = np.zeros((n, n))
    right = np.block([[q.T, zero, zero, q.T], [zero, q.T, q.T, zero]])
    even, odd = q[0::2], q[1::2]
    left = np.block([[even[:, 0::2], even[:, 1::2]], [odd[:, 1::2], odd[:, 0::2]]])
    return right.astype(np.float32), left.astype(np.float32)


def dot(a, b):
    return jnp.dot(a, b, precision=EXACT, preferred_element_type=jnp.float32)


def plane_transform(slabs, right, left):
    rows = slabs[0].shape[0]
    wide = dot(jnp.concatenate(slabs, axis=0), right)
    count = len(slabs)
    straight = [wide[i * rows : (i + 1) * rows, :LANES] for i in range(count)]
    swapped = [wide[i * rows : (i + 1) * rows, LANES:] for i in range(count)]
    tall = jnp.concatenate(
        [jnp.concatenate(straight, axis=1), jnp.concatenate(swapped, axis=1)], axis=0
    )
    both = dot(left, tall)
    low = lax.broadcasted_iota(jnp.int32, (rows, LANES), 1) < LANES // 2
    return [
        jnp.where(
            low,
            both[:rows, i * LANES : (i + 1) * LANES],
            both[rows:, i * LANES : (i + 1) * LANES],
        )
        for i in range(count)
    ]


def lane_of(shape):
    return lax.broadcasted_iota(jnp.int32, shape, 1)


def y_behind(v):
    half = LANES // 2
    r = pltpu.roll(v, half, 1)
    return jnp.where(lane_of(v.shape) < half, pltpu.roll(r, 1, 0), r)


def y_ahead(v):
    half = LANES // 2
    r = pltpu.roll(v, half, 1)
    return jnp.where(lane_of(v.shape) < half, r, pltpu.roll(r, v.shape[0] - 1, 0))


def z_behind(v):
    half = LANES // 2
    edge = lane_of(v.shape) % half == 0
    return jnp.where(edge, pltpu.roll(v, half + 1, 1), pltpu.roll(v, 1, 1))


def z_ahead(v):
    half = LANES // 2
    edge = lane_of(v.shape) % half == half - 1
    return jnp.where(edge, pltpu.roll(v, half - 1, 1), pltpu.roll(v, LANES - 1, 1))


def project(get):
    pairs = ((0, 1), (0, 2), (1, 2))
    out = [0.5 * (get(0, a, b) - get(0, b, a)) for a, b in pairs]
    out += [0.5 * (get(1, a, b) + get(1, b, a)) for a, b in pairs]
    diag = [get(1, a, a) for a in range(3)]
    third = (diag[0] + diag[1] + diag[2]) * (1.0 / 3.0)
    return out + [diag[0] - third, diag[1] - third]


def cmul(a, b):
    return (a[0] * b[0] - a[1] * b[1], a[0] * b[1] + a[1] * b[0])


def exponential(fields):
    v = [STEP * f for f in fields]
    h0, h1 = v[6], v[7]
    h2 = -(h0 + h1)
    h01, h02, h12 = (v[3], -v[0]), (v[4], -v[1]), (v[5], -v[2])
    n01 = h01[0] * h01[0] + h01[1] * h01[1]
    n02 = h02[0] * h02[0] + h02[1] * h02[1]
    n12 = h12[0] * h12[0] + h12[1] * h12[1]
    c = 0.5 * (h0 * h0 + h1 * h1 + h2 * h2) + n01 + n02 + n12
    prod = cmul(h01, h12)
    triple = prod[0] * h02[0] + prod[1] * h02[1]
    d = h0 * h1 * h2 + 2.0 * triple - h0 * n12 - h1 * n02 - h2 * n01
    cd, cc, dd = c * d, c * c, d * d
    f0 = (1.0 - dd * (1 / 720), cd * (1 / 120) - d * (1 / 6))
    f1 = (d * (1 / 24) - cd * (1 / 360), 1.0 - c * (1 / 6) + cc * (1 / 120))
    f2 = (c * (1 / 24) - 0.5 - cc * (1 / 720), d * (1 / 120))
    for _ in range(3):
        s00, s01, s02 = cmul(f0, f0), cmul(f0, f1), cmul(f0, f2)
        s11, s12, s22 = cmul(f1, f1), cmul(f1, f2), cmul(f2, f2)
        f0 = tuple(s00[i] + 2.0 * d * s12[i] for i in range(2))
        f1 = tuple(2.0 * (s01[i] + c * s12[i]) + d * s22[i] for i in range(2))
        f2 = tuple(s11[i] + 2.0 * s02[i] + c * s22[i] for i in range(2))
    conj = lambda x: (x[0], -x[1])
    mixed = cmul(h02, conj(h12))
    q01 = (mixed[0] - h2 * h01[0], mixed[1] - h2 * h01[1])
    q02 = (prod[0] - h1 * h02[0], prod[1] - h1 * h02[1])
    mixed = cmul(conj(h01), h02)
    q12 = (mixed[0] - h0 * h12[0], mixed[1] - h0 * h12[1])
    diag = ((h0, h0 * h0 + n01 + n02), (h1, h1 * h1 + n01 + n12), (h2, h2 * h2 + n02 + n12))
    gauge = [[None] * 3 for _ in range(3)]
    for a in range(3):
        h, q = diag[a]
        gauge[a][a] = tuple(f0[i] + f1[i] * h + f2[i] * q for i in range(2))
    for a, b, h, q in ((0, 1, h01, q01), (0, 2, h02, q02), (1, 2, h12, q12)):
        x, y = cmul(f1, h), cmul(f2, q)
        gauge[a][b] = (x[0] + y[0], x[1] + y[1])
        x, y = cmul(f1, conj(h)), cmul(f2, conj(q))
        gauge[b][a] = (x[0] + y[0], x[1] + y[1])
    return gauge


def matmul3(left, right, adjoint=False):
    out = [[None] * 3 for _ in range(3)]
    for a in range(3):
        for b in range(3):
            re = im = None
            for k in range(3):
                xr, xi = left[a][k]
                yr, yi = right[b][k] if adjoint else right[k][b]
                if adjoint:
                    r, i = xr * yr + xi * yi, xi * yr - xr * yi
                else:
                    r, i = xr * yr - xi * yi, xr * yi + xi * yr
                re, im = (r, i) if re is None else (re + r, im + i)
            out[a][b] = (re, im)
    return out


def at(part, a, b):
    return part * 9 + a * 3 + b


def forward(u, planes, right, left, slab_ref, chunk_ref):
    slabs = [[None] * (planes + 1) for _ in range(FIELDS)]
    for p in range(planes):
        along = [
            project(lambda part, a, b, i=i: u(i, part, a, b, p)) for i in range(3)
        ]
        for f in range(FIELDS):
            value = (
                y_behind(along[1][f]) - along[1][f] + z_behind(along[2][f]) - along[2][f]
            ) - along[0][f]
            if p > 0:
                value = value + slabs[f][planes]
            slabs[f][p] = value
            slabs[f][planes] = along[0][f]
    flat = [slabs[f][p] for f in range(FIELDS) for p in range(planes + 1)]
    done = plane_transform(flat, right, left)
    for i, slab in enumerate(done):
        slab_ref[i] = slab
    depth = chunk_ref.shape[2] // FIELDS
    for d in range(chunk_ref.shape[0]):
        for p in range(planes + 1):
            for f in range(FIELDS):
                chunk_ref[d, p, f * depth : (f + 1) * depth, :] = slab_ref[
                    f * (planes + 1) + p, d * depth : (d + 1) * depth, :
                ]


def backward(recv_ref, planes, right, left, slab_ref):
    depth = recv_ref.shape[2] // FIELDS
    for s in range(recv_ref.shape[0]):
        for p in range(planes + 1):
            for f in range(FIELDS):
                slab_ref[f * (planes + 1) + p, s * depth : (s + 1) * depth, :] = recv_ref[
                    s, p, f * depth : (f + 1) * depth, :
                ]
    done = plane_transform(
        [slab_ref[i] for i in range(FIELDS * (planes + 1))], right, left
    )
    for i, slab in enumerate(done):
        slab_ref[i] = slab


def first_kernel(planes, links_ref, right_ref, left_ref, chunk_ref, slab_ref):
    rows = links_ref.shape[1] // planes

    def u(i, part, a, b, p):
        return links_ref[i * 18 + at(part, a, b), pl.ds(p, rows, planes), :]

    forward(u, planes, right_ref[...], left_ref[...], slab_ref, chunk_ref)


def across_kernel(basis, moment, planes, recv_ref, yz_ref, send_ref):
    count = recv_ref.shape[0]
    n = basis.shape[0]
    for j in range(recv_ref.shape[2] // 8):
        band = slice(j * 8, j * 8 + 8)
        yz = yz_ref[band, :]
        v = []
        for s in range(count):
            for p in range(planes):
                value = recv_ref[s, p, band, :]
                if p == 0:
                    value = value + recv_ref[(s - 1) % count, planes, band, :]
                v.append(value)
        half = range(1, (n + 1) // 2)
        even = {0: v[0]}
        odd = {}
        if n % 2 == 0:
            even[n // 2] = v[n // 2]
        for x in half:
            even[x] = v[x] + v[n - x]
            odd[x] = v[x] - v[n - x]
        back_even = {x: None for x in even}
        back_odd = {x: None for x in odd}
        for k in range(n):
            is_sine = abs(basis[k, 0]) < 1e-9
            source, target = (odd, back_odd) if is_sine else (even, back_even)
            mode = None
            for x in source:
                term = float(basis[k, x]) * source[x]
                mode = term if mode is None else mode + term
            p2 = yz + float(moment[k])
            if moment[k] == 0.0:
                weight = jnp.where(p2 > 0.0, PEAK / jnp.where(p2 > 0.0, p2, 1.0), 0.0)
            else:
                weight = PEAK / p2
            mode = mode * weight
            for x in target:
                term = float(basis[k, x]) * mode
                target[x] = term if target[x] is None else target[x] + term
        g = [None] * n
        for x in back_even:
            g[x] = back_even[x]
        for x in half:
            g[x] = back_even[x] + back_odd[x]
            g[n - x] = back_even[x] - back_odd[x]
        for d in range(count):
            for p in range(planes + 1):
                send_ref[d, p, band, :] = g[(d * planes + p) % n]


def gauge_of(slab_ref, planes, gauge_ref):
    rows = gauge_ref.shape[2]

    for p in range(planes + 1):

        @pl.loop(0, rows // 8)
        def _(j):
            band = pl.ds(pl.multiple_of(j * 8, 8), 8)
            g = exponential([slab_ref[f * (planes + 1) + p, band, :] for f in range(FIELDS)])
            for a in range(3):
                for b in range(3):
                    for part in range(2):
                        gauge_ref[at(part, a, b), p, band, :] = g[a][b][part]


def rotate_all(get_band, put_band, planes, gauge_ref, ahead_ref):
    rows = gauge_ref.shape[2]
    for e in range(18):
        for p in range(planes):
            ahead_ref[e, p] = y_ahead(gauge_ref[e, p])
            ahead_ref[18 + e, p] = z_ahead(gauge_ref[e, p])
    for p in range(planes):

        @pl.loop(0, rows // 8)
        def _(j):
            start = pl.multiple_of(j * 8, 8)
            band = pl.ds(start, 8)
            for i in range(3):
                g = [
                    [tuple(gauge_ref[at(r, a, b), p, band, :] for r in range(2)) for b in range(3)]
                    for a in range(3)
                ]
                u = [
                    [tuple(get_band(i, r, a, b, p, j) for r in range(2)) for b in range(3)]
                    for a in range(3)
                ]
                if i == 0:
                    source = lambda r, a, b: gauge_ref[at(r, a, b), p + 1, band, :]
                else:
                    source = lambda r, a, b: ahead_ref[(i - 1) * 18 + at(r, a, b), p, band, :]
                ahead = [
                    [tuple(source(r, a, b) for r in range(2)) for b in range(3)]
                    for a in range(3)
                ]
                out = matmul3(matmul3(g, u), ahead, adjoint=True)
                for a in range(3):
                    for b in range(3):
                        for r in range(2):
                            put_band(i, r, a, b, p, j, out[a][b][r])


def middle_kernel(
    planes, strided, recv_ref, links_ref, right_ref, left_ref, back_ref, turn_ref,
    out_ref, field_ref, chunk_ref, slab_ref, gauge_ref, ahead_ref,
):
    backward(recv_ref, planes, back_ref[...], turn_ref[...], slab_ref)
    for f in range(FIELDS):
        for p in range(planes):
            field_ref[f * planes + p] = slab_ref[f * (planes + 1) + p]
    gauge_of(slab_ref, planes, gauge_ref)

    def get(i, r, a, b, p, j):
        if strided:
            return links_ref[i * 18 + at(r, a, b), pl.ds(j * 8 * planes + p, 8, planes), :]
        return links_ref[i * 18 + at(r, a, b), p, pl.ds(pl.multiple_of(j * 8, 8), 8), :]

    def put(i, r, a, b, p, j, value):
        out_ref[i * 18 + at(r, a, b), p, pl.ds(pl.multiple_of(j * 8, 8), 8), :] = value

    rotate_all(get, put, planes, gauge_ref, ahead_ref)

    def u(i, part, a, b, p):
        return out_ref[i * 18 + at(part, a, b), p]

    forward(u, planes, right_ref[...], left_ref[...], slab_ref, chunk_ref)


def fields_kernel(planes, recv_ref, back_ref, turn_ref, slab_ref, field_ref):
    backward(recv_ref, planes, back_ref[...], turn_ref[...], slab_ref)
    for f in range(FIELDS):
        for p in range(planes):
            field_ref[f * planes + p] = slab_ref[f * (planes + 1) + p]


def last_kernel(planes, slab_ref, links_ref, out_ref, gauge_ref, ahead_ref):
    gauge_of(slab_ref, planes, gauge_ref)

    def get(i, r, a, b, p, j):
        return links_ref[i * 18 + at(r, a, b), p, pl.ds(pl.multiple_of(j * 8, 8), 8), :]

    def put(i, r, a, b, p, j, value):
        out_ref[i * 18 + at(r, a, b), pl.ds(j * 8 * planes + p, 8, planes), :] = value

    rotate_all(get, put, planes, gauge_ref, ahead_ref)


def sink_kernel(
    planes, scalar_ref, own_one_ref, own_two_ref, all_one_ref, all_two_ref, prop_ref,
    out_ref, acc_ref, sum_ref,
):
    rows = own_one_ref.shape[1]
    sink, present, plane, row, lane = (scalar_ref[i] for i in range(5))
    pairs = prop_ref.shape[0] // 2
    acc_ref[...] = jnp.zeros_like(acc_ref)
    sum_ref[...] = jnp.zeros_like(sum_ref)

    for p in range(planes):

        @pl.loop(0, rows // 8)
        def _(j):
            band = pl.ds(pl.multiple_of(j * 8, 8), 8)
            one = exponential([all_one_ref[sink, f * planes + p, band, :] for f in range(FIELDS)])
            two = exponential([all_two_ref[sink, f * planes + p, band, :] for f in range(FIELDS)])
            t = matmul3(two, one)
            for q in range(pairs // 3):
                s = [
                    tuple(
                        prop_ref[r * pairs + q * 3 + k, pl.ds(j * 8 * planes + p, 8, planes), :]
                        for r in range(2)
                    )
                    for k in range(3)
                ]
                for a in range(3):
                    re = im = None
                    for k in range(3):
                        x = cmul(t[a][k], s[k])
                        re, im = x if re is None else (re + x[0], im + x[1])
                    acc_ref[q * 3 + a] += re
                    acc_ref[pairs + q * 3 + a] += im

    spot = (lax.broadcasted_iota(jnp.int32, (rows, LANES), 0) == row) & (
        lax.broadcasted_iota(jnp.int32, (rows, LANES), 1) == lane
    )

    def pick(ref, f):
        total = jnp.zeros((1, 1), jnp.float32)
        for p in range(planes):
            here = spot & (plane == p)
            total = total + jnp.sum(jnp.where(here, ref[f * planes + p], 0.0), keepdims=True)
        return jnp.broadcast_to(total, (8, LANES))

    anchor = matmul3(
        exponential([pick(own_two_ref, f) for f in range(FIELDS)]),
        exponential([pick(own_one_ref, f) for f in range(FIELDS)]),
    )
    first = lane_of((1, LANES)) == 0
    for e in range(2 * pairs):
        sum_ref[e : e + 1, :] = jnp.sum(acc_ref[e], axis=0, keepdims=True)
    for r in range(2):
        for a in range(3):
            for b in range(3):
                e = 2 * pairs + at(r, a, b)
                sum_ref[e : e + 1, :] = jnp.where(
                    first & (present > 0), anchor[a][b][r][0:1, :], 0.0
                )
    out_ref[...] = lax.dot_general(
        jnp.ones((8, LANES), jnp.float32),
        sum_ref[...],
        (((1,), (1,)), ((), ())),
        precision=EXACT,
        preferred_element_type=jnp.float32,
    )


def exchange_kernel(plan, sizes, *refs):
    n = len(plan)
    sources, targets = refs[:n], refs[n : 2 * n]
    local_sem = refs[2 * n]
    sems = refs[2 * n + 1 :]
    barrier = pltpu.get_barrier_semaphore()
    axes = sorted(set(axis for axis, _ in plan))
    greeted = 0
    for axis in axes:
        me = lax.axis_index(axis)
        for off in range(1, sizes[axis]):
            peer = lax.rem(me + off, sizes[axis])
            pl.semaphore_signal(barrier, inc=1, device_id={axis: peer}, device_id_type=MESH)
            greeted += 1
    pl.semaphore_wait(barrier, greeted)
    copies = []
    for i, (axis, scatter) in enumerate(plan):
        size = sizes[axis]
        me = lax.axis_index(axis)
        for off in range(1, size):
            peer = lax.rem(me + off, size)
            copy = pltpu.make_async_remote_copy(
                src_ref=sources[i].at[peer] if scatter else sources[i],
                dst_ref=targets[i].at[me],
                send_sem=sems[2 * i].at[off],
                recv_sem=sems[2 * i + 1].at[off],
                device_id={axis: peer},
                device_id_type=MESH,
            )
            copy.start()
            copies.append(copy)
    for i, (axis, scatter) in enumerate(plan):
        me = lax.axis_index(axis)
        copy = pltpu.make_async_copy(
            sources[i].at[me] if scatter else sources[i], targets[i].at[me], local_sem.at[i]
        )
        copy.start()
        copies.append(copy)
    for copy in copies:
        copy.wait()


def exchange(arrays, plan, sizes, collective_id):
    outs, sems = [], []
    for array, (axis, scatter) in zip(arrays, plan):
        shape = array.shape if scatter else (sizes[axis],) + array.shape
        outs.append(jax.ShapeDtypeStruct(shape, jnp.float32))
        sems += [pltpu.SemaphoreType.DMA((sizes[axis],))] * 2
    return pl.pallas_call(
        functools.partial(exchange_kernel, tuple(plan), sizes),
        out_shape=outs,
        in_specs=[VMEM] * len(arrays),
        out_specs=[VMEM] * len(arrays),
        scratch_shapes=[pltpu.SemaphoreType.DMA((len(arrays),))] + sems,
        compiler_params=pltpu.CompilerParams(
            collective_id=collective_id, has_side_effects=True, vmem_limit_bytes=LIMIT
        ),
    )(*arrays)


def local(kernel, outs, scratch, args, smem=0):
    return pl.pallas_call(
        kernel,
        out_shape=[jax.ShapeDtypeStruct(s, jnp.float32) for s in outs],
        in_specs=[SMEM] * smem + [VMEM] * (len(args) - smem),
        out_specs=[VMEM] * len(outs),
        scratch_shapes=[pltpu.VMEM(s, jnp.float32) for s in scratch],
        compiler_params=pltpu.CompilerParams(vmem_limit_bytes=LIMIT),
    )(*args)


def body(sizes, links, propagator, sink_time, src_time, src_site):
    space, times = sizes["space"], sizes["tm"]
    planes, area = links.shape[5], links.shape[6]
    side = math.isqrt(area)
    across = planes * space
    rows = area // LANES
    depth = rows // space
    assert side * 2 == LANES and rows % space == 0 and rows % 8 == 0

    basis, moment = real_basis(side)
    right, left = plane_matrices(basis)
    back, turn = plane_matrices(basis.T)
    x_basis, x_moment = real_basis(across)
    yz = (moment.reshape(rows, 2, 1) + moment[None, None, :]).reshape(rows, LANES)
    yz = np.tile(yz.reshape(space, 1, depth, LANES), (1, FIELDS, 1, 1))
    yz = yz.reshape(space, FIELDS * depth, LANES).astype(np.float32)

    space_index = lax.axis_index("space")
    time_index = lax.axis_index("tm")
    yz = lax.dynamic_index_in_dim(jnp.asarray(yz), space_index, 0, keepdims=False)

    def fold(x):
        lead = x.shape[:-2]
        x = x.reshape(lead + (planes, rows, LANES))
        return jnp.swapaxes(x, -3, -2).reshape((-1, rows * planes, LANES))

    linked = fold(links[0])
    slab = (FIELDS * (planes + 1), rows, LANES)
    field = (FIELDS * planes, rows, LANES)
    chunk = (space, planes + 1, FIELDS * depth, LANES)
    gauge = (18, planes + 1, rows, LANES)
    ahead = (36, planes, rows, LANES)
    split = (54, planes, rows, LANES)

    def across_all(received):
        kernel = functools.partial(across_kernel, x_basis, x_moment, planes)
        return local(kernel, [chunk], [], [received, yz])[0]

    (send,) = local(
        functools.partial(first_kernel, planes), [chunk], [slab], [linked, right, left]
    )
    fields = []
    gathered = []
    lattice = linked
    cid = 0
    for sweep in range(ITERS):
        arrays, plan = [send], [("space", True)]
        if fields:
            arrays.append(fields[-1])
            plan.append(("tm", False))
        got = exchange(arrays, plan, sizes, cid)
        gathered += got[1:]
        (got,) = exchange([across_all(got[0])], [("space", True)], sizes, cid + 1)
        cid += 2
        if sweep < ITERS - 1:
            kernel = functools.partial(middle_kernel, planes, sweep == 0)
            lattice, a_field, send = local(
                kernel,
                [split, field, chunk],
                [slab, gauge, ahead],
                [got, lattice, right, left, back, turn],
            )
        else:
            slabs, a_field = local(
                functools.partial(fields_kernel, planes), [slab, field], [], [got, back, turn]
            )
        fields.append(a_field)
    gathered += exchange([fields[-1]], [("tm", False)], sizes, cid)
    (final,) = local(
        functools.partial(last_kernel, planes),
        [(54, rows * planes, LANES)],
        [gauge, ahead],
        [slabs, lattice],
    )
    final = jnp.swapaxes(final.reshape(54, rows, planes, LANES), 1, 2)
    final = final.reshape(links.shape)

    site = src_site[0]
    plane = site // area - space_index * planes
    column = site % area
    present = (src_time[0] % times == time_index) & (plane >= 0) & (plane < planes)
    scalars = jnp.stack(
        [
            sink_time[0] % times,
            present.astype(jnp.int32),
            plane,
            column // LANES,
            column % LANES,
        ]
    )
    pairs = propagator.shape[1]
    depth_sum = LANES * -(-(2 * pairs + 18) // LANES)
    assert depth_sum == LANES
    (partial,) = local(
        functools.partial(sink_kernel, planes),
        [(8, LANES)],
        [(2 * pairs, 8, LANES), (depth_sum, LANES)],
        [scalars, fields[0], fields[1], gathered[0], gathered[1], fold(propagator)],
        smem=1,
    )
    (over_space,) = exchange([partial], [("space", False)], sizes, cid + 1)
    over_space = jnp.sum(over_space, axis=0)
    (over_time,) = exchange([over_space], [("tm", False)], sizes, cid + 2)
    table = over_time[:, 0, :]
    summed = table[:, : 2 * pairs].reshape(times, 2, pairs)
    summed = jnp.swapaxes(summed, 0, 1).reshape(2, 4, 3, SC)
    anchor = jnp.sum(table[:, 2 * pairs : 2 * pairs + 18], axis=0).reshape(2, 3, 3)
    left_re, left_im = summed[0][:, None], summed[1][:, None]
    right_re, right_im = (anchor[i][None, :, :, None] for i in range(2))
    real = jnp.sum(left_re * right_re + left_im * right_im, axis=2)
    imag = jnp.sum(left_im * right_re - left_re * right_im, axis=2)
    wall = jnp.stack([real.reshape(SC * SC), imag.reshape(SC * SC)])
    return final, wall * float(across * area) ** (-0.5)


def solution(mesh):
    sizes = {axis: mesh.shape[axis] for axis in ("space", "tm")}
    placed = (
        P("tm", None, None, None, None, "space", None),
        P(None, "tm", "space", None),
        P(),
        P(),
        P(),
    )
    return jax.shard_map(
        functools.partial(body, sizes),
        mesh=mesh,
        in_specs=placed,
        out_specs=(P("tm", None, None, None, None, "space", None), P()),
        check_vma=False,
    )
```

```python
import functools
import math

import jax
import jax.numpy as jnp
import numpy as np
from jax import lax
from jax.experimental import pallas as pl
from jax.experimental.pallas import tpu as pltpu
from jax.sharding import PartitionSpec as P

SC = 12
ITERS = 2
STEP = 0.08 / 16.0
PEAK = 12.0
LANES = 128
FIELDS = 8
EXACT = lax.Precision.HIGHEST
MESH = pl.DeviceIdType.MESH
VMEM = pl.BlockSpec(memory_space=pltpu.VMEM)
SMEM = pl.BlockSpec(memory_space=pltpu.SMEM)
LIMIT = 60 * 1024 * 1024


def real_basis(n):
    x = np.arange(n)
    rows, moment = [], []
    for k in range(n // 2 + 1):
        angle = 2.0 * np.pi * ((k * x) % n) / n
        square = 4.0 * np.sin(np.pi * k / n) ** 2
        if k == 0 or 2 * k == n:
            rows.append(np.cos(angle) / np.sqrt(n))
            moment.append(square)
        else:
            rows.append(np.cos(angle) * np.sqrt(2.0 / n))
            rows.append(np.sin(angle) * np.sqrt(2.0 / n))
            moment += [square, square]
    return np.array(rows), np.array(moment)


def plane_matrices(q):
    n = q.shape[0]
    zero = np.zeros((n, n))
    right = np.block([[q.T, zero, zero, q.T], [zero, q.T, q.T, zero]])
    even, odd = q[0::2], q[1::2]
    left = np.block([[even[:, 0::2], even[:, 1::2]], [odd[:, 1::2], odd[:, 0::2]]])
    return right.astype(np.float32), left.astype(np.float32)


def dot(a, b):
    return jnp.dot(a, b, precision=EXACT, preferred_element_type=jnp.float32)


def plane_transform(slabs, right, left):
    rows = slabs[0].shape[0]
    wide = dot(jnp.concatenate(slabs, axis=0), right)
    count = len(slabs)
    straight = [wide[i * rows : (i + 1) * rows, :LANES] for i in range(count)]
    swapped = [wide[i * rows : (i + 1) * rows, LANES:] for i in range(count)]
    tall = jnp.concatenate(
        [jnp.concatenate(straight, axis=1), jnp.concatenate(swapped, axis=1)], axis=0
    )
    both = dot(left, tall)
    low = lax.broadcasted_iota(jnp.int32, (rows, LANES), 1) < LANES // 2
    return [
        jnp.where(
            low,
            both[:rows, i * LANES : (i + 1) * LANES],
            both[rows:, i * LANES : (i + 1) * LANES],
        )
        for i in range(count)
    ]


def lane_of(shape):
    return lax.broadcasted_iota(jnp.int32, shape, 1)


def y_behind(v):
    half = LANES // 2
    r = pltpu.roll(v, half, 1)
    return jnp.where(lane_of(v.shape) < half, pltpu.roll(r, 1, 0), r)


def y_ahead(v):
    half = LANES // 2
    r = pltpu.roll(v, half, 1)
    return jnp.where(lane_of(v.shape) < half, r, pltpu.roll(r, v.shape[0] - 1, 0))


def z_behind(v):
    half = LANES // 2
    edge = lane_of(v.shape) % half == 0
    return jnp.where(edge, pltpu.roll(v, half + 1, 1), pltpu.roll(v, 1, 1))


def z_ahead(v):
    half = LANES // 2
    edge = lane_of(v.shape) % half == half - 1
    return jnp.where(edge, pltpu.roll(v, half - 1, 1), pltpu.roll(v, LANES - 1, 1))


def project(get):
    pairs = ((0, 1), (0, 2), (1, 2))
    out = [0.5 * (get(0, a, b) - get(0, b, a)) for a, b in pairs]
    out += [0.5 * (get(1, a, b) + get(1, b, a)) for a, b in pairs]
    diag = [get(1, a, a) for a in range(3)]
    third = (diag[0] + diag[1] + diag[2]) * (1.0 / 3.0)
    return out + [diag[0] - third, diag[1] - third]


def cmul(a, b):
    return (a[0] * b[0] - a[1] * b[1], a[0] * b[1] + a[1] * b[0])


def exponential(fields):
    v = [STEP * f for f in fields]
    h0, h1 = v[6], v[7]
    h2 = -(h0 + h1)
    h01, h02, h12 = (v[3], -v[0]), (v[4], -v[1]), (v[5], -v[2])
    n01 = h01[0] * h01[0] + h01[1] * h01[1]
    n02 = h02[0] * h02[0] + h02[1] * h02[1]
    n12 = h12[0] * h12[0] + h12[1] * h12[1]
    c = 0.5 * (h0 * h0 + h1 * h1 + h2 * h2) + n01 + n02 + n12
    prod = cmul(h01, h12)
    triple = prod[0] * h02[0] + prod[1] * h02[1]
    d = h0 * h1 * h2 + 2.0 * triple - h0 * n12 - h1 * n02 - h2 * n01
    cd, cc, dd = c * d, c * c, d * d
    f0 = (1.0 - dd * (1 / 720), cd * (1 / 120) - d * (1 / 6))
    f1 = (d * (1 / 24) - cd * (1 / 360), 1.0 - c * (1 / 6) + cc * (1 / 120))
    f2 = (c * (1 / 24) - 0.5 - cc * (1 / 720), d * (1 / 120))
    for _ in range(3):
        s00, s01, s02 = cmul(f0, f0), cmul(f0, f1), cmul(f0, f2)
        s11, s12, s22 = cmul(f1, f1), cmul(f1, f2), cmul(f2, f2)
        f0 = tuple(s00[i] + 2.0 * d * s12[i] for i in range(2))
        f1 = tuple(2.0 * (s01[i] + c * s12[i]) + d * s22[i] for i in range(2))
        f2 = tuple(s11[i] + 2.0 * s02[i] + c * s22[i] for i in range(2))
    conj = lambda x: (x[0], -x[1])
    mixed = cmul(h02, conj(h12))
    q01 = (mixed[0] - h2 * h01[0], mixed[1] - h2 * h01[1])
    q02 = (prod[0] - h1 * h02[0], prod[1] - h1 * h02[1])
    mixed = cmul(conj(h01), h02)
    q12 = (mixed[0] - h0 * h12[0], mixed[1] - h0 * h12[1])
    diag = ((h0, h0 * h0 + n01 + n02), (h1, h1 * h1 + n01 + n12), (h2, h2 * h2 + n02 + n12))
    gauge = [[None] * 3 for _ in range(3)]
    for a in range(3):
        h, q = diag[a]
        gauge[a][a] = tuple(f0[i] + f1[i] * h + f2[i] * q for i in range(2))
    for a, b, h, q in ((0, 1, h01, q01), (0, 2, h02, q02), (1, 2, h12, q12)):
        x, y = cmul(f1, h), cmul(f2, q)
        gauge[a][b] = (x[0] + y[0], x[1] + y[1])
        x, y = cmul(f1, conj(h)), cmul(f2, conj(q))
        gauge[b][a] = (x[0] + y[0], x[1] + y[1])
    return gauge


def matmul3(left, right, adjoint=False):
    out = [[None] * 3 for _ in range(3)]
    for a in range(3):
        for b in range(3):
            re = im = None
            for k in range(3):
                xr, xi = left[a][k]
                yr, yi = right[b][k] if adjoint else right[k][b]
                if adjoint:
                    r, i = xr * yr + xi * yi, xi * yr - xr * yi
                else:
                    r, i = xr * yr - xi * yi, xr * yi + xi * yr
                re, im = (r, i) if re is None else (re + r, im + i)
            out[a][b] = (re, im)
    return out


def at(part, a, b):
    return part * 9 + a * 3 + b


def forward(u, planes, right, left, slab_ref, chunk_ref):
    slabs = [[None] * (planes + 1) for _ in range(FIELDS)]
    for p in range(planes):
        along = [
            project(lambda part, a, b, i=i: u(i, part, a, b, p)) for i in range(3)
        ]
        for f in range(FIELDS):
            value = (
                y_behind(along[1][f]) - along[1][f] + z_behind(along[2][f]) - along[2][f]
            ) - along[0][f]
            if p > 0:
                value = value + slabs[f][planes]
            slabs[f][p] = value
            slabs[f][planes] = along[0][f]
    flat = [slabs[f][p] for f in range(FIELDS) for p in range(planes + 1)]
    done = plane_transform(flat, right, left)
    for i, slab in enumerate(done):
        slab_ref[i] = slab
    depth = chunk_ref.shape[2] // FIELDS
    for d in range(chunk_ref.shape[0]):
        for p in range(planes + 1):
            for f in range(FIELDS):
                chunk_ref[d, p, f * depth : (f + 1) * depth, :] = slab_ref[
                    f * (planes + 1) + p, d * depth : (d + 1) * depth, :
                ]


def backward(recv_ref, planes, right, left, slab_ref):
    depth = recv_ref.shape[2] // FIELDS
    for s in range(recv_ref.shape[0]):
        for p in range(planes + 1):
            for f in range(FIELDS):
                slab_ref[f * (planes + 1) + p, s * depth : (s + 1) * depth, :] = recv_ref[
                    s, p, f * depth : (f + 1) * depth, :
                ]
    done = plane_transform(
        [slab_ref[i] for i in range(FIELDS * (planes + 1))], right, left
    )
    for i, slab in enumerate(done):
        slab_ref[i] = slab


def first_kernel(planes, links_ref, right_ref, left_ref, chunk_ref, slab_ref):
    rows = links_ref.shape[1] // planes

    def u(i, part, a, b, p):
        return links_ref[i * 18 + at(part, a, b), pl.ds(p, rows, planes), :]

    forward(u, planes, right_ref[...], left_ref[...], slab_ref, chunk_ref)


def across_kernel(basis, moment, planes, recv_ref, yz_ref, send_ref):
    count = recv_ref.shape[0]
    n = basis.shape[0]
    for j in range(recv_ref.shape[2] // 8):
        band = slice(j * 8, j * 8 + 8)
        yz = yz_ref[band, :]
        v = []
        for s in range(count):
            for p in range(planes):
                value = recv_ref[s, p, band, :]
                if p == 0:
                    value = value + recv_ref[(s - 1) % count, planes, band, :]
                v.append(value)
        half = range(1, (n + 1) // 2)
        even = {0: v[0]}
        odd = {}
        if n % 2 == 0:
            even[n // 2] = v[n // 2]
        for x in half:
            even[x] = v[x] + v[n - x]
            odd[x] = v[x] - v[n - x]
        back_even = {x: None for x in even}
        back_odd = {x: None for x in odd}
        for k in range(n):
            is_sine = abs(basis[k, 0]) < 1e-9
            source, target = (odd, back_odd) if is_sine else (even, back_even)
            mode = None
            for x in source:
                term = float(basis[k, x]) * source[x]
                mode = term if mode is None else mode + term
            p2 = yz + float(moment[k])
            if moment[k] == 0.0:
                weight = jnp.where(p2 > 0.0, PEAK / jnp.where(p2 > 0.0, p2, 1.0), 0.0)
            else:
                weight = PEAK / p2
            mode = mode * weight
            for x in target:
                term = float(basis[k, x]) * mode
                target[x] = term if target[x] is None else target[x] + term
        g = [None] * n
        for x in back_even:
            g[x] = back_even[x]
        for x in half:
            g[x] = back_even[x] + back_odd[x]
            g[n - x] = back_even[x] - back_odd[x]
        for d in range(count):
            for p in range(planes + 1):
                send_ref[d, p, band, :] = g[(d * planes + p) % n]


def gauge_of(slab_ref, planes, gauge_ref):
    rows = gauge_ref.shape[2]

    for p in range(planes + 1):

        @pl.loop(0, rows // 8)
        def _(j):
            band = pl.ds(pl.multiple_of(j * 8, 8), 8)
            g = exponential([slab_ref[f * (planes + 1) + p, band, :] for f in range(FIELDS)])
            for a in range(3):
                for b in range(3):
                    for part in range(2):
                        gauge_ref[at(part, a, b), p, band, :] = g[a][b][part]


def rotate_all(get_band, put_band, planes, gauge_ref, ahead_ref):
    rows = gauge_ref.shape[2]
    for e in range(18):
        for p in range(planes):
            ahead_ref[e, p] = y_ahead(gauge_ref[e, p])
            ahead_ref[18 + e, p] = z_ahead(gauge_ref[e, p])
    for p in range(planes):

        @pl.loop(0, rows // 8)
        def _(j):
            start = pl.multiple_of(j * 8, 8)
            band = pl.ds(start, 8)
            for i in range(3):
                g = [
                    [tuple(gauge_ref[at(r, a, b), p, band, :] for r in range(2)) for b in range(3)]
                    for a in range(3)
                ]
                u = [
                    [tuple(get_band(i, r, a, b, p, j) for r in range(2)) for b in range(3)]
                    for a in range(3)
                ]
                if i == 0:
                    source = lambda r, a, b: gauge_ref[at(r, a, b), p + 1, band, :]
                else:
                    source = lambda r, a, b: ahead_ref[(i - 1) * 18 + at(r, a, b), p, band, :]
                ahead = [
                    [tuple(source(r, a, b) for r in range(2)) for b in range(3)]
                    for a in range(3)
                ]
                out = matmul3(matmul3(g, u), ahead, adjoint=True)
                for a in range(3):
                    for b in range(3):
                        for r in range(2):
                            put_band(i, r, a, b, p, j, out[a][b][r])


def middle_kernel(
    planes, strided, recv_ref, links_ref, right_ref, left_ref, back_ref, turn_ref,
    out_ref, field_ref, chunk_ref, slab_ref, gauge_ref, ahead_ref,
):
    backward(recv_ref, planes, back_ref[...], turn_ref[...], slab_ref)
    for f in range(FIELDS):
        for p in range(planes):
            field_ref[f * planes + p] = slab_ref[f * (planes + 1) + p]
    gauge_of(slab_ref, planes, gauge_ref)

    def get(i, r, a, b, p, j):
        if strided:
            return links_ref[i * 18 + at(r, a, b), pl.ds(j * 8 * planes + p, 8, planes), :]
        return links_ref[i * 18 + at(r, a, b), p, pl.ds(pl.multiple_of(j * 8, 8), 8), :]

    def put(i, r, a, b, p, j, value):
        out_ref[i * 18 + at(r, a, b), p, pl.ds(pl.multiple_of(j * 8, 8), 8), :] = value

    rotate_all(get, put, planes, gauge_ref, ahead_ref)

    def u(i, part, a, b, p):
        return out_ref[i * 18 + at(part, a, b), p]

    forward(u, planes, right_ref[...], left_ref[...], slab_ref, chunk_ref)


def fields_kernel(planes, recv_ref, back_ref, turn_ref, slab_ref, field_ref):
    backward(recv_ref, planes, back_ref[...], turn_ref[...], slab_ref)
    for f in range(FIELDS):
        for p in range(planes):
            field_ref[f * planes + p] = slab_ref[f * (planes + 1) + p]


def last_kernel(planes, slab_ref, links_ref, out_ref, gauge_ref, ahead_ref):
    gauge_of(slab_ref, planes, gauge_ref)

    def get(i, r, a, b, p, j):
        return links_ref[i * 18 + at(r, a, b), p, pl.ds(pl.multiple_of(j * 8, 8), 8), :]

    def put(i, r, a, b, p, j, value):
        out_ref[i * 18 + at(r, a, b), pl.ds(j * 8 * planes + p, 8, planes), :] = value

    rotate_all(get, put, planes, gauge_ref, ahead_ref)


def sink_kernel(
    planes, scalar_ref, own_one_ref, own_two_ref, all_one_ref, all_two_ref, prop_ref,
    out_ref, acc_ref, sum_ref,
):
    rows = own_one_ref.shape[1]
    present, plane, row, lane = (scalar_ref[i] for i in range(4))
    pairs = prop_ref.shape[0] // 2
    acc_ref[...] = jnp.zeros_like(acc_ref)
    sum_ref[...] = jnp.zeros_like(sum_ref)

    for p in range(planes):

        @pl.loop(0, rows // 8)
        def _(j):
            band = pl.ds(pl.multiple_of(j * 8, 8), 8)
            one = exponential([all_one_ref[f * planes + p, band, :] for f in range(FIELDS)])
            two = exponential([all_two_ref[f * planes + p, band, :] for f in range(FIELDS)])
            t = matmul3(two, one)
            for q in range(pairs // 3):
                s = [
                    tuple(
                        prop_ref[r * pairs + q * 3 + k, pl.ds(j * 8 * planes + p, 8, planes), :]
                        for r in range(2)
                    )
                    for k in range(3)
                ]
                for a in range(3):
                    re = im = None
                    for k in range(3):
                        x = cmul(t[a][k], s[k])
                        re, im = x if re is None else (re + x[0], im + x[1])
                    acc_ref[q * 3 + a] += re
                    acc_ref[pairs + q * 3 + a] += im

    spot = (lax.broadcasted_iota(jnp.int32, (rows, LANES), 0) == row) & (
        lax.broadcasted_iota(jnp.int32, (rows, LANES), 1) == lane
    )

    def pick(ref, f):
        total = jnp.zeros((1, 1), jnp.float32)
        for p in range(planes):
            here = spot & (plane == p)
            total = total + jnp.sum(jnp.where(here, ref[f * planes + p], 0.0), keepdims=True)
        return jnp.broadcast_to(total, (8, LANES))

    anchor = matmul3(
        exponential([pick(own_two_ref, f) for f in range(FIELDS)]),
        exponential([pick(own_one_ref, f) for f in range(FIELDS)]),
    )
    first = lane_of((1, LANES)) == 0
    for e in range(2 * pairs):
        sum_ref[e : e + 1, :] = jnp.sum(acc_ref[e], axis=0, keepdims=True)
    for r in range(2):
        for a in range(3):
            for b in range(3):
                e = 2 * pairs + at(r, a, b)
                sum_ref[e : e + 1, :] = jnp.where(
                    first & (present > 0), anchor[a][b][r][0:1, :], 0.0
                )
    out_ref[...] = lax.dot_general(
        jnp.ones((8, LANES), jnp.float32),
        sum_ref[...],
        (((1,), (1,)), ((), ())),
        precision=EXACT,
        preferred_element_type=jnp.float32,
    )[0:1, :]


def greet(axis, offsets, sizes):
    barrier = pltpu.get_barrier_semaphore()
    me = lax.axis_index(axis)
    for off in offsets:
        peer = lax.rem(me + off, sizes[axis])
        pl.semaphore_signal(barrier, inc=1, device_id={axis: peer}, device_id_type=MESH)
    return len(offsets)


def scatter_start(source, target, send, recv, local_sem, sizes, copies):
    size = sizes["space"]
    me = lax.axis_index("space")
    for off in range(1, size):
        peer = lax.rem(me + off, size)
        copy = pltpu.make_async_remote_copy(
            src_ref=source.at[peer],
            dst_ref=target.at[me],
            send_sem=send.at[off],
            recv_sem=recv.at[off],
            device_id={"space": peer},
            device_id_type=MESH,
        )
        copy.start()
        copies.append(copy)
    copy = pltpu.make_async_copy(source.at[me], target.at[me], local_sem)
    copy.start()
    copies.append(copy)


def relay(source, target, up, down, recv, local_sem, root, sizes):
    size = sizes["tm"]
    me = lax.axis_index("tm")
    count = source.shape[0]

    @pl.when(me == root)
    def _():
        copy = pltpu.make_async_copy(source, target, local_sem)
        copy.start()
        copy.wait()

    def hop(k, sem, step):
        return pltpu.make_async_remote_copy(
            src_ref=target.at[k],
            dst_ref=target.at[k],
            send_sem=sem.at[k],
            recv_sem=recv.at[k],
            device_id={"tm": lax.rem(me + step, size)},
            device_id_type=MESH,
        )

    rises = (me >= root) & (me < size - 1)
    falls = (me <= root) & (me > 0)
    for k in range(count):

        @pl.when(me != root)
        def _():
            hop(k, up, 1).wait_recv()

        @pl.when(rises)
        def _():
            hop(k, up, 1).start()

        @pl.when(falls)
        def _():
            hop(k, down, size - 1).start()

    for k in range(count):

        @pl.when(rises)
        def _():
            hop(k, up, 1).wait_send()

        @pl.when(falls)
        def _():
            hop(k, down, size - 1).wait_send()


def exchange_kernel(sizes, root, scatter, *refs):
    refs = list(refs)
    n = int(scatter) + int(root is not None)
    sources, targets, sems = refs[:n], refs[n : 2 * n], refs[2 * n :]
    total = 0
    if scatter:
        total += greet("space", range(1, sizes["space"]), sizes)
    if root is not None:
        total += greet("tm", (1, sizes["tm"] - 1), sizes)
    pl.semaphore_wait(pltpu.get_barrier_semaphore(), total)
    copies = []
    if scatter:
        scatter_start(sources[0], targets[0], sems[0], sems[1], sems[2], sizes, copies)
        sems = sems[3:]
    if root is not None:
        relay(sources[-1], targets[-1], sems[0], sems[1], sems[2], sems[3], root, sizes)
    for copy in copies:
        copy.wait()


def exchange(arrays, sizes, collective_id, scatter=True, root=None):
    sems = []
    if scatter:
        sems += [pltpu.SemaphoreType.DMA((sizes["space"],))] * 2 + [pltpu.SemaphoreType.DMA]
    if root is not None:
        count = arrays[-1].shape[0]
        sems += [pltpu.SemaphoreType.DMA((count,))] * 3 + [pltpu.SemaphoreType.DMA]
    return pl.pallas_call(
        functools.partial(exchange_kernel, sizes, root, scatter),
        out_shape=[jax.ShapeDtypeStruct(a.shape, jnp.float32) for a in arrays],
        in_specs=[VMEM] * len(arrays),
        out_specs=[VMEM] * len(arrays),
        scratch_shapes=sems,
        compiler_params=pltpu.CompilerParams(
            collective_id=collective_id, has_side_effects=True, vmem_limit_bytes=LIMIT
        ),
    )(*arrays)


def gather_kernel(sizes, axes, source, target, send, recv, local_sem):
    me = [lax.axis_index(axis) for axis in axes]
    extent = [sizes[axis] for axis in axes]
    slot = 0
    for index, size in zip(me, extent):
        slot = slot * size + index
    barrier = pltpu.get_barrier_semaphore()
    peers = []
    for flat in range(1, math.prod(extent)):
        rest, peer = flat, {}
        for axis, index, size in reversed(list(zip(axes, me, extent))):
            peer[axis] = lax.rem(index + rest % size, size)
            rest //= size
        peers.append((flat, peer))
    for _, peer in peers:
        pl.semaphore_signal(barrier, inc=1, device_id=peer, device_id_type=MESH)
    pl.semaphore_wait(barrier, len(peers))
    copies = []
    for flat, peer in peers:
        copy = pltpu.make_async_remote_copy(
            src_ref=source,
            dst_ref=target.at[slot],
            send_sem=send.at[flat],
            recv_sem=recv.at[flat],
            device_id=peer,
            device_id_type=MESH,
        )
        copy.start()
        copies.append(copy)
    copy = pltpu.make_async_copy(source, target.at[slot], local_sem)
    copy.start()
    copies.append(copy)
    for copy in copies:
        copy.wait()


def gather(row, axes, sizes, collective_id):
    count = math.prod(sizes[axis] for axis in axes)
    return pl.pallas_call(
        functools.partial(gather_kernel, sizes, axes),
        out_shape=jax.ShapeDtypeStruct((count,) + row.shape, jnp.float32),
        in_specs=[VMEM],
        out_specs=VMEM,
        scratch_shapes=[pltpu.SemaphoreType.DMA((count,))] * 2 + [pltpu.SemaphoreType.DMA],
        compiler_params=pltpu.CompilerParams(collective_id=collective_id, has_side_effects=True),
    )(row)


def local(kernel, outs, scratch, args, smem=0):
    return pl.pallas_call(
        kernel,
        out_shape=[jax.ShapeDtypeStruct(s, jnp.float32) for s in outs],
        in_specs=[SMEM] * smem + [VMEM] * (len(args) - smem),
        out_specs=[VMEM] * len(outs),
        scratch_shapes=[pltpu.VMEM(s, jnp.float32) for s in scratch],
        compiler_params=pltpu.CompilerParams(vmem_limit_bytes=LIMIT),
    )(*args)


def body(sizes, links, propagator, sink_time, src_time, src_site):
    space, times = sizes["space"], sizes["tm"]
    planes, area = links.shape[5], links.shape[6]
    side = math.isqrt(area)
    across = planes * space
    rows = area // LANES
    depth = rows // space
    assert side * 2 == LANES and rows % space == 0 and rows % 8 == 0

    basis, moment = real_basis(side)
    right, left = plane_matrices(basis)
    back, turn = plane_matrices(basis.T)
    x_basis, x_moment = real_basis(across)
    yz = (moment.reshape(rows, 2, 1) + moment[None, None, :]).reshape(rows, LANES)
    yz = np.tile(yz.reshape(space, 1, depth, LANES), (1, FIELDS, 1, 1))
    yz = yz.reshape(space, FIELDS * depth, LANES).astype(np.float32)

    space_index = lax.axis_index("space")
    time_index = lax.axis_index("tm")
    yz = lax.dynamic_index_in_dim(jnp.asarray(yz), space_index, 0, keepdims=False)

    def fold(x):
        lead = x.shape[:-2]
        x = x.reshape(lead + (planes, rows, LANES))
        return jnp.swapaxes(x, -3, -2).reshape((-1, rows * planes, LANES))

    linked = fold(links[0])
    slab = (FIELDS * (planes + 1), rows, LANES)
    field = (FIELDS * planes, rows, LANES)
    chunk = (space, planes + 1, FIELDS * depth, LANES)
    gauge = (18, planes + 1, rows, LANES)
    ahead = (36, planes, rows, LANES)
    split = (54, planes, rows, LANES)

    def across_all(received):
        kernel = functools.partial(across_kernel, x_basis, x_moment, planes)
        return local(kernel, [chunk], [], [received, yz])[0]

    (send,) = local(
        functools.partial(first_kernel, planes), [chunk], [slab], [linked, right, left]
    )
    fields = []
    spread = []
    lattice = linked
    sink = sink_time[0] % times
    for sweep in range(ITERS):
        if sweep == 0:
            (got,) = exchange([send], sizes, 0)
        else:
            got, field_one = lax.switch(
                sink,
                [
                    functools.partial(
                        lambda root, x, y: exchange([x, y], sizes, 8 + root, root=root), root
                    )
                    for root in range(times)
                ],
                send,
                fields[-1],
            )
            spread.append(field_one)
        (got,) = exchange([across_all(got)], sizes, 1 + sweep)
        if sweep < ITERS - 1:
            kernel = functools.partial(middle_kernel, planes, sweep == 0)
            lattice, a_field, send = local(
                kernel,
                [split, field, chunk],
                [slab, gauge, ahead],
                [got, lattice, right, left, back, turn],
            )
        else:
            slabs, a_field = local(
                functools.partial(fields_kernel, planes), [slab, field], [], [got, back, turn]
            )
        fields.append(a_field)
    (field_two,) = lax.switch(
        sink,
        [
            functools.partial(
                lambda root, x: exchange(
                    [x], sizes, 8 + times + root, scatter=False, root=root
                ),
                root,
            )
            for root in range(times)
        ],
        fields[-1],
    )
    spread.append(field_two)
    (final,) = local(
        functools.partial(last_kernel, planes),
        [(54, rows * planes, LANES)],
        [gauge, ahead],
        [slabs, lattice],
    )
    final = jnp.swapaxes(final.reshape(54, rows, planes, LANES), 1, 2)
    final = final.reshape(links.shape)

    site = src_site[0]
    plane = site // area - space_index * planes
    column = site % area
    present = (src_time[0] % times == time_index) & (plane >= 0) & (plane < planes)
    scalars = jnp.stack(
        [
            present.astype(jnp.int32),
            plane,
            column // LANES,
            column % LANES,
        ]
    )
    pairs = propagator.shape[1]
    depth_sum = LANES * -(-(2 * pairs + 18) // LANES)
    assert depth_sum == LANES
    (partial,) = local(
        functools.partial(sink_kernel, planes),
        [(1, LANES)],
        [(2 * pairs, 8, LANES), (depth_sum, LANES)],
        [scalars, fields[0], fields[1], spread[0], spread[1], fold(propagator)],
        smem=1,
    )
    if space * times <= 64:
        every = gather(partial, ("space", "tm"), sizes, 3)
        table = jnp.sum(every.reshape(space, times, LANES), axis=0)
    else:
        over_space = jnp.sum(gather(partial, ("space",), sizes, 3), axis=0)
        table = gather(over_space, ("tm",), sizes, 4)[:, 0, :]
    summed = table[:, : 2 * pairs].reshape(times, 2, pairs)
    summed = jnp.swapaxes(summed, 0, 1).reshape(2, 4, 3, SC)
    anchor = jnp.sum(table[:, 2 * pairs : 2 * pairs + 18], axis=0).reshape(2, 3, 3)
    left_re, left_im = summed[0][:, None], summed[1][:, None]
    right_re, right_im = (anchor[i][None, :, :, None] for i in range(2))
    real = jnp.sum(left_re * right_re + left_im * right_im, axis=2)
    imag = jnp.sum(left_im * right_re - left_re * right_im, axis=2)
    wall = jnp.stack([real.reshape(SC * SC), imag.reshape(SC * SC)])
    return final, wall * float(across * area) ** (-0.5)


def solution(mesh):
    sizes = {axis: mesh.shape[axis] for axis in ("space", "tm")}
    placed = (
        P("tm", None, None, None, None, "space", None),
        P(None, "tm", "space", None),
        P(),
        P(),
        P(),
    )
    return jax.shard_map(
        functools.partial(body, sizes),
        mesh=mesh,
        in_specs=placed,
        out_specs=(P("tm", None, None, None, None, "space", None), P()),
        check_vma=False,
    )
```
